32 devices in a mesh: grp: 8 (over z, x), dom: 4 (over y, core).
Axes of the slice: x: 2, y: 2, z: 4, core: 2. Of those that a mesh axis runs over, the one named last changes fastest.
Arguments:
- positions: float32 [3, 4096, 512], P(None, ('grp', 'dom')), may hold values from 0 to 1
- velocities: float32 [3, 4096, 512], P(None, ('grp', 'dom')), may hold values from -6 to 6
- masses: float32 [4096, 512], P(('grp', 'dom')), may hold values from 0.5 to 2
- block_halo: int32 [4096], P(('grp', 'dom')), may hold values from 0 to 4095, as said below
- block_shift: int32 [3, 4096], P(None, ('grp', 'dom')), may hold values from -1 to 1
- block_live: int32 [4096], P(('grp', 'dom')), may hold values from 64 to 512
- block_count: int32 [32], P(('grp', 'dom')), may hold values from 32 to 128
- home_slot: int32 [4096], replicated, may hold values from 0 to 4095, as said below
Outputs:
- halo_table: float32 [11, 4096], P(None, ('grp', 'dom'))
- kinetic: float32 [4096, 512], P(('grp', 'dom'))
- radial: float32 [4096, 512], P(('grp', 'dom'))
The draws below stay inside these ranges and needn't reach their ends.
Inputs may be any that keep to these rules, and one draw needn't show every extreme that they name: A permutation: the halo h is owned by the device of index home_slot[h] // 128 (grp+dom order), in its column home_slot[h] % 128. `block_halo`: the owner of a block's halo lies in the block's own index of grp or in the next one (index + 1, wrapping around); both occur.
All inputs are finite; a program needn't handle non-finite values.
Results may differ from the reference program's by a relative error of at most 0.0003.
Values sent between devices are 32-bit elements; how exact they have to be, the bound alone decides.
No kernel may reach another device: no remote copies, remote signals or barrier semaphores. Data moves between devices by JAX's collectives and lax.ppermute only.
A program may use at most 64 MiB of HBM per device.

```python
import math
import jax
import jax.numpy as jnp
from jax import lax

BS = 512
BLK_DEV = 128
HALO_DEV = 128
NB = 4096
HALOS = 4096
N_GRP = 8
N_DOM = 4
DEVICES = 32


def owner_table(key):
    return jax.random.permutation(jax.random.fold_in(key, 11), HALOS).astype(jnp.int32)


def draw_home_slot(key, part):
    return owner_table(key)


def draw_block_halo(key, part):
    home = owner_table(key)
    inverse = jnp.argsort(home).astype(jnp.int32)
    window = N_DOM * HALO_DEV
    first_key, second_key, third_key = jax.random.split(jax.random.fold_in(key, 23), 3)
    limit = jax.random.randint(first_key, (NB,), 1, 2 * window + 1)
    picked = jax.random.randint(second_key, (NB,), 0, limit)
    mixing = jax.random.permutation(third_key, 2 * window).astype(jnp.int32)
    picked = mixing[picked]
    group_index = jnp.arange(NB, dtype=jnp.int32) // BLK_DEV // N_DOM
    column = (group_index + picked // window) % N_GRP * window + picked % window
    return inverse[column].astype(jnp.int32)


def touch_ends(values, rng, least, top_value):
    extent = values.shape
    spot = [jax.random.randint(jax.random.fold_in(rng, axis), (), 0, extent[axis]) for axis in range(len(extent))]
    values = values.at[tuple(spot)].set(least)
    longest = extent.index(max(extent))
    spot[longest] = (spot[longest] + 1) % extent[longest]
    return values.at[tuple(spot)].set(top_value)


def steps_of(rng, dims, cuts, smallest, top_value):
    level = 1.0
    for axis_at, shards_of in cuts:
        draws = jax.random.uniform(jax.random.fold_in(jax.random.fold_in(rng, 6), axis_at), (shards_of,), jnp.float32, smallest / len(cuts), top_value / len(cuts))
        level = level * jnp.repeat(jnp.exp(draws), dims[axis_at] // shards_of).reshape((-1,) + (1,) * (len(dims) - 1 - axis_at))
    return level


def normal_values(own_key, extent, scale, bound, pieces=(), kind=jnp.bfloat16):
    entries = scale * jax.random.normal(own_key, extent, jnp.float32)
    if pieces:
        entries = entries * steps_of(own_key, extent, pieces, -0.22, 0.18)
    return jnp.clip(entries, -bound, bound).astype(kind)


def setup_inputs(seed: int = 0) -> dict:
    key_of = jax.random.split(jax.random.key(seed), 9)
    positions = jnp.clip(1.0 * jax.random.uniform(key_of[0], (3, NB, BS), jnp.float32) ** steps_of(key_of[0], (3, NB, BS), ((1, 32),), -0.2, 0.2), 0.0, 1.0)
    velocities = normal_values(key_of[1], (3, NB, BS), 1.0, 6.0, ((1, 32),), jnp.float32)
    masses = jnp.clip(jnp.exp(math.log(2.0) - 1.3862944 * jax.random.uniform(key_of[2], (NB, BS), jnp.float32) ** steps_of(key_of[2], (NB, BS), ((0, 32),), -0.2, 0.2)), 0.5, 2.0)
    block_halo = draw_block_halo(jax.random.fold_in(key_of[8], 71), 0)
    block_shift = touch_ends(jax.random.randint(key_of[4], (3, NB), -1, 2), jax.random.fold_in(key_of[4], 1), -1, 1).astype(jnp.int32)
    block_live = touch_ends(jax.random.randint(key_of[5], (NB,), BS // 8, BS + 1), jax.random.fold_in(key_of[5], 1), BS // 8, BS).astype(jnp.int32)
    block_count = touch_ends(jax.random.randint(key_of[6], (DEVICES,), max(1, BLK_DEV // 4), BLK_DEV + 1), jax.random.fold_in(key_of[6], 1), max(1, BLK_DEV // 4), BLK_DEV).astype(jnp.int32)
    home_slot = draw_home_slot(jax.random.fold_in(key_of[8], 71), 0)
    return {"positions": positions, "velocities": velocities, "masses": masses, "block_halo": block_halo, "block_shift": block_shift, "block_live": block_live, "block_count": block_count, "home_slot": home_slot}


BOX = 1.0
EPSILON = 1e-6


def crossed(first, second):
    return jnp.stack([first[1] * second[2] - first[2] * second[1],
                      first[2] * second[0] - first[0] * second[2],
                      first[0] * second[1] - first[1] * second[0]])


def block_moments(positions, velocities, masses, block_shift, block_live, valid):
    lanes = jnp.arange(masses.shape[1], dtype=jnp.int32)
    live_mask = ((lanes[None, :] < block_live[:, None]) & valid[:, None]).astype(masses.dtype)
    weights = masses * live_mask
    unwrapped = positions + BOX * block_shift.astype(positions.dtype)[:, :, None]
    speed_sq = jnp.sum(velocities * velocities, axis=0)
    angular = crossed(unwrapped, velocities)
    rows = [jnp.sum(weights, axis=1)[None], jnp.sum(weights * unwrapped, axis=2),
            jnp.sum(weights * velocities, axis=2), jnp.sum(weights * speed_sq, axis=1)[None],
            jnp.sum(weights * angular, axis=2)]
    return jnp.concatenate(rows, axis=0), live_mask, unwrapped


def halo_properties(sums, total, halos):
    heavy = jnp.maximum(sums[0], 1.0)
    centre = sums[1:4] / heavy
    drift = sums[4:7] / heavy
    spread = sums[7] / heavy - jnp.sum(drift * drift, axis=0)
    spin = sums[8:11] / heavy - crossed(centre, drift)
    share = sums[0] * halos / total
    return jnp.concatenate([share[None], centre, drift, spread[None], spin], axis=0)


def particle_outputs(unwrapped, velocities, live_mask, stats):
    centre = stats[0:3][:, :, None]
    drift = stats[3:6][:, :, None]
    spread = stats[6][:, None]
    offset = velocities - drift
    kinetic = jnp.sum(offset * offset, axis=0) / (3.0 * spread + EPSILON)
    distance = unwrapped - centre
    radial = jnp.sum(distance * distance, axis=0)
    return kinetic * live_mask, radial * live_mask


def reference(positions, velocities, masses, block_halo, block_shift, block_live, block_count, home_slot):
    groups = block_count.shape[0]
    total_blocks = masses.shape[0]
    width = masses.shape[1]
    grouped_pos = positions.reshape(3, groups, BLK_DEV, width).transpose(1, 0, 2, 3)
    grouped_vel = velocities.reshape(3, groups, BLK_DEV, width).transpose(1, 0, 2, 3)
    grouped_mass = masses.reshape(groups, BLK_DEV, width)
    grouped_shift = block_shift.reshape(3, groups, BLK_DEV).transpose(1, 0, 2)
    grouped_live = block_live.reshape(groups, BLK_DEV)
    valid = jnp.arange(BLK_DEV, dtype=jnp.int32)[None, :] < block_count[:, None]

    def per_group(items):
        place, speed, weight, shift, alive, usable = items
        return block_moments(place, speed, weight, shift, alive, usable)[0]

    moments = lax.map(per_group, (grouped_pos, grouped_vel, grouped_mass, grouped_shift, grouped_live, valid))
    moments = moments.transpose(1, 0, 2).reshape(11, total_blocks)
    slots = home_slot[block_halo]
    halos = home_slot.shape[0]
    sums = jnp.zeros((11, halos), moments.dtype).at[:, slots].add(moments)
    total = jnp.sum(moments[0])
    halo_table = halo_properties(sums, total, halos)
    stats = halo_table[1:8][:, slots].reshape(7, groups, BLK_DEV).transpose(1, 0, 2)

    def outputs(items):
        place, speed, weight, shift, alive, usable, local_stats = items
        _, live_mask, unwrapped = block_moments(place, speed, weight, shift, alive, usable)
        return particle_outputs(unwrapped, speed, live_mask, local_stats)

    kinetic, radial = lax.map(outputs, (grouped_pos, grouped_vel, grouped_mass, grouped_shift, grouped_live, valid, stats))
    return halo_table, kinetic.reshape(total_blocks, width), radial.reshape(total_blocks, width)
```

```python
import functools

import jax
import jax.numpy as jnp
from jax import lax
from jax.experimental import pallas as pl
from jax.experimental.pallas import tpu as pltpu
from jax.sharding import PartitionSpec as P

EPSILON = 1e-06
LANES = 128
CHUNKS = 4
MOMENTS = 11
AXES = ("grp", "dom")


def rows_to_array(rows, count, width):
    at = lax.broadcasted_iota(jnp.int32, (count, width), 0)
    out = jnp.zeros((count, width), jnp.float32)
    for k, row in enumerate(rows):
        out = jnp.where(at == k, row, out)
    return out


def moments_kernel(
    pos_hbm, vel_hbm, mass_hbm, halo_ref, home_ref, shift_ref, live_ref, count_ref,
    send_ref, pos_ref, vel_ref, side_ref, cols_ref, mass_ref, acc_ref, sems,
):
    blocks, width = mass_ref.shape
    step = blocks // CHUNKS
    copies = []
    for c in range(CHUNKS):
        rows = pl.ds(c * step, step)
        copies.append(
            [
                pltpu.make_async_copy(mass_hbm.at[rows], mass_ref.at[rows], sems.at[0, c]),
                pltpu.make_async_copy(vel_hbm.at[:, rows], vel_ref.at[:, rows], sems.at[1, c]),
                pltpu.make_async_copy(pos_hbm.at[:, rows], pos_ref.at[:, rows], sems.at[2, c]),
            ]
        )
        for copy in copies[c]:
            copy.start()

    halo = halo_ref[...]
    low = lax.broadcasted_iota(jnp.int32, (LANES, blocks), 0) == halo % LANES
    picked = lax.dot_general(
        home_ref[...].astype(jnp.float32), low.astype(jnp.float32), (((1,), (0,)), ((), ())),
        precision=lax.Precision.HIGHEST, preferred_element_type=jnp.float32,
    )
    high = lax.broadcasted_iota(jnp.int32, picked.shape, 0) == halo // LANES
    slot = jnp.sum(jnp.where(high, picked, 0.0), axis=0, keepdims=True)

    at = lax.broadcasted_iota(jnp.int32, (1, blocks), 1)
    live = jnp.where(at < count_ref[0], live_ref[...], 0).astype(jnp.float32)
    shift = shift_ref[...].astype(jnp.float32)
    side = rows_to_array([live, shift[0:1], shift[1:2], shift[2:3], slot], 8, blocks)
    side_ref[...] = side
    cols = jnp.transpose(side)
    cols_ref[...] = cols

    lane = lax.broadcasted_iota(jnp.int32, (8, width), 1).astype(jnp.float32)
    lane_of = lax.broadcasted_iota(jnp.int32, (8, LANES), 1)
    for r in range(0, blocks, 8):
        if r % step == 0:
            for copy in copies[r // step]:
                copy.wait()
        rows = slice(r, r + 8)
        weight = jnp.where(lane < cols[rows, 0:1], mass_ref[rows], 0.0)
        ux, uy, uz = (pos_ref[k, rows] + cols[rows, k + 1 : k + 2] for k in range(3))
        vx, vy, vz = (vel_ref[k, rows] for k in range(3))
        mx, my, mz = weight * vx, weight * vy, weight * vz
        terms = (
            weight, weight * ux, weight * uy, weight * uz, mx, my, mz,
            mx * vx + my * vy + mz * vz,
            uy * mz - uz * my, uz * mx - ux * mz, ux * my - uy * mx,
        )
        acc = jnp.where(lane_of == MOMENTS, cols[rows, 4:5], 0.0)
        for k, term in enumerate(terms):
            acc = jnp.where(lane_of == k, jnp.sum(term, axis=1, keepdims=True), acc)
        acc_ref[rows] = acc

    table = jnp.transpose(acc_ref[...])
    for s in range(send_ref.shape[0]):
        for k in range(3):
            send_ref[s, :, k * blocks : (k + 1) * blocks] = table[4 * k : 4 * k + 4]


def outputs_kernel(
    groups, domains, halos,
    recv_ref, pos_ref, vel_ref, side_ref, cols_ref,
    table_ref, kin_hbm, rad_hbm, kin_ref, rad_ref, sems,
):
    blocks, width = kin_ref.shape
    owned = halos // (groups * domains)
    group, domain = lax.axis_index("grp"), lax.axis_index("dom")

    near = []
    for offset in sorted({o % groups for o in (-1, 0, 1)}):
        first = lax.rem(group + offset, groups) * domains
        for d in range(domains):
            part = recv_ref[first + d]
            near.append(
                jnp.concatenate([part[:, k * blocks : (k + 1) * blocks] for k in range(3)], axis=0)
            )
    base = ((group * domains + domain) * owned).astype(jnp.float32)
    mine = jnp.broadcast_to(cols_ref[:, 4:5], (blocks, LANES))
    own = lax.broadcasted_iota(jnp.int32, (owned, LANES), 0).astype(jnp.float32) + base
    want = jnp.concatenate([mine, own], axis=0)
    same = jnp.concatenate(
        [jnp.where(want == rows[MOMENTS : MOMENTS + 1], 1.0, 0.0).astype(jnp.bfloat16) for rows in near],
        axis=1,
    )
    values = jnp.concatenate(near, axis=1)
    values = jnp.concatenate([values, jnp.zeros((4, values.shape[1]), jnp.float32)], axis=0)
    top = values.astype(jnp.bfloat16)
    rest = values - top.astype(jnp.float32)
    mid = rest.astype(jnp.bfloat16)
    last = (rest - mid.astype(jnp.float32)).astype(jnp.bfloat16)
    sums = lax.dot_general(
        jnp.concatenate([top, mid, last], axis=0), same, (((1,), (1,)), ((), ())),
        preferred_element_type=jnp.float32,
    )
    sums = sums[0:16] + sums[16:32] + sums[32:48]

    heavy = jnp.maximum(sums[0:1], 1.0)
    mean = sums[0:8] / heavy
    cx, cy, cz, dx, dy, dz, energy = (mean[k : k + 1] for k in range(1, 8))
    spread = energy - (dx * dx + dy * dy + dz * dz)

    m = slice(0, blocks)
    side = side_ref[...]
    stats = rows_to_array(
        [
            cx[:, m] - side[1:2], cy[:, m] - side[2:3], cz[:, m] - side[3:4],
            dx[:, m], dy[:, m], dz[:, m], 1.0 / (3.0 * spread[:, m] + EPSILON),
        ],
        8, blocks,
    )
    stats = jnp.transpose(stats)
    cols = cols_ref[...]
    lane = lax.broadcasted_iota(jnp.int32, (8, width), 1).astype(jnp.float32)
    step = blocks // CHUNKS
    copies = []
    for r in range(0, blocks, 8):
        rows = slice(r, r + 8)
        alive = lane < cols[rows, 0:1]
        rx, ry, rz = (pos_ref[k, rows] - stats[rows, k : k + 1] for k in range(3))
        ox, oy, oz = (vel_ref[k, rows] - stats[rows, k + 3 : k + 4] for k in range(3))
        kinetic = (ox * ox + oy * oy + oz * oz) * stats[rows, 6:7]
        kin_ref[rows] = jnp.where(alive, kinetic, 0.0)
        rad_ref[rows] = jnp.where(alive, rx * rx + ry * ry + rz * rz, 0.0)
        if (r + 8) % step == 0:
            c = r // step
            part = pl.ds(c * step, step)
            for k, (src, dst) in enumerate(((kin_ref, kin_hbm), (rad_ref, rad_hbm))):
                copies.append(pltpu.make_async_copy(src.at[part], dst.at[part], sems.at[k, c]))
                copies[-1].start()

    whole = jnp.zeros((4, blocks), jnp.float32)
    for s in range(recv_ref.shape[0]):
        whole = whole + recv_ref[s, :, 0:blocks]
    total = jnp.sum(whole[0:1], axis=1, keepdims=True)
    o = slice(blocks, blocks + owned)
    share = sums[0:1, o] * float(halos) / total
    at = lax.broadcasted_iota(jnp.int32, (8, owned), 0)
    table_ref[0:8] = jnp.where(at == 0, share, jnp.where(at == 7, spread[:, o], mean[:, o]))
    cx, cy, cz, dx, dy, dz = (v[:, o] for v in (cx, cy, cz, dx, dy, dz))
    turn = rows_to_array([cy * dz - cz * dy, cz * dx - cx * dz, cx * dy - cy * dx], 8, owned)
    table_ref[8:11] = (sums[8:16, o] / heavy[:, o] - turn)[0:3]
    for copy in copies:
        copy.wait()


def local(positions, velocities, masses, block_halo, block_shift, block_live, block_count, home_slot):
    blocks, width = masses.shape
    halos = home_slot.shape[0]
    groups, domains = lax.axis_size("grp"), lax.axis_size("dom")
    devices = groups * domains
    anywhere = pl.BlockSpec(memory_space=pl.ANY)
    vmem = pl.BlockSpec(memory_space=pltpu.VMEM)
    send, pos, vel, side, cols = pl.pallas_call(
        moments_kernel,
        out_shape=(
            pltpu.VMEM((devices, 4, 3 * blocks), jnp.float32),
            pltpu.VMEM(positions.shape, jnp.float32),
            pltpu.VMEM(velocities.shape, jnp.float32),
            pltpu.VMEM((8, blocks), jnp.float32),
            pltpu.VMEM((blocks, 8), jnp.float32),
        ),
        in_specs=[anywhere] * 3 + [vmem] * 4 + [pl.BlockSpec(memory_space=pltpu.SMEM)],
        out_specs=(vmem,) * 5,
        scratch_shapes=[
            pltpu.VMEM((blocks, width), jnp.float32),
            pltpu.VMEM((blocks, LANES), jnp.float32),
            pltpu.SemaphoreType.DMA((3, CHUNKS)),
        ],
        compiler_params=pltpu.CompilerParams(vmem_limit_bytes=16 * 1024 * 1024),
        name="moments",
    )(
        positions, velocities, masses, block_halo.reshape(1, blocks),
        home_slot.reshape(halos // LANES, LANES), block_shift, block_live.reshape(1, blocks), block_count,
    )
    recv = lax.all_to_all(send, AXES, 0, 0)
    table, kinetic, radial = pl.pallas_call(
        functools.partial(outputs_kernel, groups, domains, halos),
        out_shape=(
            jax.ShapeDtypeStruct((MOMENTS, halos // devices), jnp.float32),
            jax.ShapeDtypeStruct((blocks, width), jnp.float32),
            jax.ShapeDtypeStruct((blocks, width), jnp.float32),
        ),
        in_specs=[vmem] * 5,
        out_specs=(vmem, anywhere, anywhere),
        scratch_shapes=[
            pltpu.VMEM((blocks, width), jnp.float32),
            pltpu.VMEM((blocks, width), jnp.float32),
            pltpu.SemaphoreType.DMA((2, CHUNKS)),
        ],
        compiler_params=pltpu.CompilerParams(vmem_limit_bytes=16 * 1024 * 1024),
        name="outputs",
    )(recv, pos, vel, side, cols)
    return table, kinetic, radial


def solution(mesh):
    return jax.shard_map(
        local,
        mesh=mesh,
        in_specs=(
            P(None, AXES, None), P(None, AXES, None), P(AXES, None), P(AXES),
            P(None, AXES), P(AXES), P(AXES), P(),
        ),
        out_specs=(P(None, AXES), P(AXES, None), P(AXES, None)),
        check_vma=False,
    )
```

```python
import functools

import jax
import jax.numpy as jnp
from jax import lax
from jax.experimental import pallas as pl
from jax.experimental.pallas import tpu as pltpu
from jax.sharding import PartitionSpec as P

EPSILON = 1e-06
LANES = 128
CHUNKS = 4
MOMENTS = 11
AXES = ("grp", "dom")


def rows_to_array(rows, count, width):
    at = lax.broadcasted_iota(jnp.int32, (count, width), 0)
    out = jnp.zeros((count, width), jnp.float32)
    for k, row in enumerate(rows):
        out = jnp.where(at == k, row, out)
    return out


def moments_kernel(
    pos_hbm, vel_hbm, mass_hbm, halo_hbm, home_hbm, shift_hbm, live_hbm, count_hbm,
    send_ref, pos_ref, vel_ref, side_ref, cols_ref, mass_ref, acc_ref,
    halo_ref, home_ref, shift_ref, live_ref, count_ref, sems, small_sems,
):
    blocks, width = mass_ref.shape
    step = blocks // CHUNKS
    small = [
        pltpu.make_async_copy(src, dst, small_sems.at[k])
        for k, (src, dst) in enumerate(
            (
                (count_hbm, count_ref), (halo_hbm, halo_ref), (home_hbm, home_ref),
                (shift_hbm, shift_ref), (live_hbm, live_ref),
            )
        )
    ]
    for copy in small:
        copy.start()
    copies = []
    for c in range(CHUNKS):
        rows = pl.ds(c * step, step)
        copies.append(
            [
                pltpu.make_async_copy(mass_hbm.at[rows], mass_ref.at[rows], sems.at[0, c]),
                pltpu.make_async_copy(vel_hbm.at[:, rows], vel_ref.at[:, rows], sems.at[1, c]),
                pltpu.make_async_copy(pos_hbm.at[:, rows], pos_ref.at[:, rows], sems.at[2, c]),
            ]
        )
        for copy in copies[c]:
            copy.start()

    for copy in small:
        copy.wait()

    halo = halo_ref[...]
    low = lax.broadcasted_iota(jnp.int32, (LANES, blocks), 0) == halo % LANES
    picked = lax.dot_general(
        home_ref[...].astype(jnp.float32), low.astype(jnp.float32), (((1,), (0,)), ((), ())),
        precision=lax.Precision.HIGHEST, preferred_element_type=jnp.float32,
    )
    high = lax.broadcasted_iota(jnp.int32, picked.shape, 0) == halo // LANES
    slot = jnp.sum(jnp.where(high, picked, 0.0), axis=0, keepdims=True)

    at = lax.broadcasted_iota(jnp.int32, (1, blocks), 1)
    live = jnp.where(at < count_ref[0], live_ref[...], 0).astype(jnp.float32)
    shift = shift_ref[...].astype(jnp.float32)
    side = rows_to_array([live, shift[0:1], shift[1:2], shift[2:3], slot], 8, blocks)
    side_ref[...] = side
    cols = jnp.transpose(side)
    cols_ref[...] = cols

    lane = lax.broadcasted_iota(jnp.int32, (8, width), 1).astype(jnp.float32)
    lane_of = lax.broadcasted_iota(jnp.int32, (8, LANES), 1)
    for r in range(0, blocks, 8):
        if r % step == 0:
            for copy in copies[r // step]:
                copy.wait()
        rows = slice(r, r + 8)
        weight = jnp.where(lane < cols[rows, 0:1], mass_ref[rows], 0.0)
        ux, uy, uz = (pos_ref[k, rows] + cols[rows, k + 1 : k + 2] for k in range(3))
        vx, vy, vz = (vel_ref[k, rows] for k in range(3))
        mx, my, mz = weight * vx, weight * vy, weight * vz
        terms = (
            weight, weight * ux, weight * uy, weight * uz, mx, my, mz,
            mx * vx + my * vy + mz * vz,
            uy * mz - uz * my, uz * mx - ux * mz, ux * my - uy * mx,
        )
        acc = jnp.where(lane_of == MOMENTS, cols[rows, 4:5], 0.0)
        for k, term in enumerate(terms):
            acc = jnp.where(lane_of == k, jnp.sum(term, axis=1, keepdims=True), acc)
        acc_ref[rows] = acc

    table = jnp.transpose(acc_ref[...])
    for s in range(send_ref.shape[0]):
        for k in range(3):
            send_ref[s, :, k * blocks : (k + 1) * blocks] = table[4 * k : 4 * k + 4]


def outputs_kernel(
    groups, domains, halos,
    recv_ref, pos_ref, vel_ref, side_ref, cols_ref,
    table_ref, kin_hbm, rad_hbm, kin_ref, rad_ref, sems,
):
    blocks, width = kin_ref.shape
    owned = halos // (groups * domains)
    group, domain = lax.axis_index("grp"), lax.axis_index("dom")

    near = []
    for offset in sorted({o % groups for o in (-1, 0, 1)}):
        first = lax.rem(group + offset, groups) * domains
        for d in range(domains):
            part = recv_ref[first + d]
            near.append(
                jnp.concatenate([part[:, k * blocks : (k + 1) * blocks] for k in range(3)], axis=0)
            )
    base = ((group * domains + domain) * owned).astype(jnp.float32)
    mine = jnp.broadcast_to(cols_ref[:, 4:5], (blocks, LANES))
    own = lax.broadcasted_iota(jnp.int32, (owned, LANES), 0).astype(jnp.float32) + base
    want = jnp.concatenate([mine, own], axis=0)
    same = jnp.concatenate(
        [jnp.where(want == rows[MOMENTS : MOMENTS + 1], 1.0, 0.0).astype(jnp.bfloat16) for rows in near],
        axis=1,
    )
    values = jnp.concatenate(near, axis=1)
    values = jnp.concatenate([values, jnp.zeros((4, values.shape[1]), jnp.float32)], axis=0)
    top = values.astype(jnp.bfloat16)
    rest = values - top.astype(jnp.float32)
    mid = rest.astype(jnp.bfloat16)
    last = (rest - mid.astype(jnp.float32)).astype(jnp.bfloat16)
    sums = lax.dot_general(
        jnp.concatenate([top, mid, last], axis=0), same, (((1,), (1,)), ((), ())),
        preferred_element_type=jnp.float32,
    )
    sums = sums[0:16] + sums[16:32] + sums[32:48]

    heavy = jnp.maximum(sums[0:1], 1.0)
    mean = sums[0:8] / heavy
    cx, cy, cz, dx, dy, dz, energy = (mean[k : k + 1] for k in range(1, 8))
    spread = energy - (dx * dx + dy * dy + dz * dz)

    m = slice(0, blocks)
    side = side_ref[...]
    stats = rows_to_array(
        [
            cx[:, m] - side[1:2], cy[:, m] - side[2:3], cz[:, m] - side[3:4],
            dx[:, m], dy[:, m], dz[:, m], 1.0 / (3.0 * spread[:, m] + EPSILON),
        ],
        8, blocks,
    )
    stats = jnp.transpose(stats)
    cols = cols_ref[...]
    lane = lax.broadcasted_iota(jnp.int32, (8, width), 1).astype(jnp.float32)
    step = blocks // CHUNKS
    copies = []
    for r in range(0, blocks, 8):
        rows = slice(r, r + 8)
        alive = lane < cols[rows, 0:1]
        rx, ry, rz = (pos_ref[k, rows] - stats[rows, k : k + 1] for k in range(3))
        ox, oy, oz = (vel_ref[k, rows] - stats[rows, k + 3 : k + 4] for k in range(3))
        kinetic = (ox * ox + oy * oy + oz * oz) * stats[rows, 6:7]
        kin_ref[rows] = jnp.where(alive, kinetic, 0.0)
        rad_ref[rows] = jnp.where(alive, rx * rx + ry * ry + rz * rz, 0.0)
        if (r + 8) % step == 0:
            c = r // step
            part = pl.ds(c * step, step)
            for k, (src, dst) in enumerate(((kin_ref, kin_hbm), (rad_ref, rad_hbm))):
                copies.append(pltpu.make_async_copy(src.at[part], dst.at[part], sems.at[k, c]))
                copies[-1].start()

    whole = jnp.zeros((4, blocks), jnp.float32)
    for s in range(recv_ref.shape[0]):
        whole = whole + recv_ref[s, :, 0:blocks]
    total = jnp.sum(whole[0:1], axis=1, keepdims=True)
    o = slice(blocks, blocks + owned)
    share = sums[0:1, o] * float(halos) / total
    at = lax.broadcasted_iota(jnp.int32, (8, owned), 0)
    table_ref[0:8] = jnp.where(at == 0, share, jnp.where(at == 7, spread[:, o], mean[:, o]))
    cx, cy, cz, dx, dy, dz = (v[:, o] for v in (cx, cy, cz, dx, dy, dz))
    turn = rows_to_array([cy * dz - cz * dy, cz * dx - cx * dz, cx * dy - cy * dx], 8, owned)
    table_ref[8:11] = (sums[8:16, o] / heavy[:, o] - turn)[0:3]
    for copy in copies:
        copy.wait()


def local(positions, velocities, masses, block_halo, block_shift, block_live, block_count, home_slot):
    blocks, width = masses.shape
    halos = home_slot.shape[0]
    groups, domains = lax.axis_size("grp"), lax.axis_size("dom")
    devices = groups * domains
    anywhere = pl.BlockSpec(memory_space=pl.ANY)
    hbm = pl.BlockSpec(memory_space=pltpu.HBM)
    vmem = pl.BlockSpec(memory_space=pltpu.VMEM)
    held = functools.partial(pltpu.with_memory_space_constraint, memory_space=pltpu.HBM)
    send, pos, vel, side, cols = pl.pallas_call(
        moments_kernel,
        out_shape=(
            pltpu.VMEM((devices, 4, 3 * blocks), jnp.float32),
            pltpu.VMEM(positions.shape, jnp.float32),
            pltpu.VMEM(velocities.shape, jnp.float32),
            pltpu.VMEM((8, blocks), jnp.float32),
            pltpu.VMEM((blocks, 8), jnp.float32),
        ),
        in_specs=[hbm] * 7 + [anywhere],
        out_specs=(vmem,) * 5,
        scratch_shapes=[
            pltpu.VMEM((blocks, width), jnp.float32),
            pltpu.VMEM((blocks, LANES), jnp.float32),
            pltpu.VMEM((1, blocks), jnp.int32),
            pltpu.VMEM((halos // LANES, LANES), jnp.int32),
            pltpu.VMEM((3, blocks), jnp.int32),
            pltpu.VMEM((1, blocks), jnp.int32),
            pltpu.SMEM((1,), jnp.int32),
            pltpu.SemaphoreType.DMA((3, CHUNKS)),
            pltpu.SemaphoreType.DMA((5,)),
        ],
        compiler_params=pltpu.CompilerParams(vmem_limit_bytes=16 * 1024 * 1024),
        name="moments",
    )(
        *map(
            held,
            (
                positions, velocities, masses, block_halo.reshape(1, blocks),
                home_slot.reshape(halos // LANES, LANES), block_shift, block_live.reshape(1, blocks),
            ),
        ),
        block_count,
    )
    recv = lax.all_to_all(send, AXES, 0, 0)
    table, kinetic, radial = pl.pallas_call(
        functools.partial(outputs_kernel, groups, domains, halos),
        out_shape=(
            jax.ShapeDtypeStruct((MOMENTS, halos // devices), jnp.float32),
            jax.ShapeDtypeStruct((blocks, width), jnp.float32),
            jax.ShapeDtypeStruct((blocks, width), jnp.float32),
        ),
        in_specs=[vmem] * 5,
        out_specs=(vmem, anywhere, anywhere),
        scratch_shapes=[
            pltpu.VMEM((blocks, width), jnp.float32),
            pltpu.VMEM((blocks, width), jnp.float32),
            pltpu.SemaphoreType.DMA((2, CHUNKS)),
        ],
        compiler_params=pltpu.CompilerParams(vmem_limit_bytes=16 * 1024 * 1024),
        name="outputs",
    )(recv, pos, vel, side, cols)
    return table, kinetic, radial


def solution(mesh):
    return jax.shard_map(
        local,
        mesh=mesh,
        in_specs=(
            P(None, AXES, None), P(None, AXES, None), P(AXES, None), P(AXES),
            P(None, AXES), P(AXES), P(AXES), P(),
        ),
        out_specs=(P(None, AXES), P(AXES, None), P(AXES, None)),
        check_vma=False,
    )
```

```python
import functools

import jax
import jax.numpy as jnp
from jax import lax
from jax.experimental import pallas as pl
from jax.experimental.pallas import tpu as pltpu
from jax.sharding import PartitionSpec as P

EPSILON = 1e-06
LANES = 128
OUT_CHUNKS = 2
MOMENTS = 11
AXES = ("grp", "dom")


def rows_to_array(rows, count, width):
    at = lax.broadcasted_iota(jnp.int32, (count, width), 0)
    out = jnp.zeros((count, width), jnp.float32)
    for k, row in enumerate(rows):
        out = jnp.where(at == k, row, out)
    return out


def moments_kernel(
    pos_hbm, vel_hbm, mass_hbm, halo_hbm, home_hbm, shift_hbm, live_hbm, count_ref,
    send_ref, pos_ref, vel_ref, side_ref, cols_ref, mass_ref, part_ref,
    halo_ref, home_ref, shift_ref, live_ref, sems, small_sems,
):
    blocks, width = mass_ref.shape
    small = [
        pltpu.make_async_copy(src, dst, small_sems.at[k])
        for k, (src, dst) in enumerate(
            (
                (halo_hbm, halo_ref), (home_hbm, home_ref), (shift_hbm, shift_ref), (live_hbm, live_ref),
            )
        )
    ]
    large = [
        pltpu.make_async_copy(src, dst, sems.at[k])
        for k, (src, dst) in enumerate(
            ((mass_hbm, mass_ref), (vel_hbm, vel_ref), (pos_hbm, pos_ref))
        )
    ]
    for copy in small + large:
        copy.start()

    for copy in small:
        copy.wait()

    halo = halo_ref[...]
    low = lax.broadcasted_iota(jnp.int32, (LANES, blocks), 0) == halo % LANES
    picked = lax.dot_general(
        home_ref[...].astype(jnp.float32), low.astype(jnp.float32), (((1,), (0,)), ((), ())),
        precision=lax.Precision.HIGHEST, preferred_element_type=jnp.float32,
    )
    high = lax.broadcasted_iota(jnp.int32, picked.shape, 0) == halo // LANES
    slot = jnp.sum(jnp.where(high, picked, 0.0), axis=0, keepdims=True)

    at = lax.broadcasted_iota(jnp.int32, (1, blocks), 1)
    live = jnp.where(at < count_ref[0], live_ref[...], 0).astype(jnp.float32)
    shift = shift_ref[...].astype(jnp.float32)
    sx, sy, sz = shift[0:1], shift[1:2], shift[2:3]
    side_ref[...] = rows_to_array([live, sx, sy, sz, slot], 8, blocks)
    cols_ref[0] = jnp.transpose(jnp.broadcast_to(live, (LANES, blocks)))
    cols_ref[1] = jnp.transpose(jnp.broadcast_to(slot, (LANES, blocks)))

    lane = lax.broadcasted_iota(jnp.int32, (8, width), 1).astype(jnp.float32)

    for copy in large:
        copy.wait()
    for r in range(0, blocks, 8):
        rows = slice(r, r + 8)
        edge = cols_ref[0, rows]
        edge = jnp.concatenate([edge] * (width // LANES), axis=1)
        weight = jnp.where(lane < edge, mass_ref[rows], 0.0)
        px, py, pz = (pos_ref[k, rows] for k in range(3))
        vx, vy, vz = (vel_ref[k, rows] for k in range(3))
        mx, my, mz = weight * vx, weight * vy, weight * vz
        terms = (
            weight, weight * px, weight * py, weight * pz, mx, my, mz,
            mx * vx + my * vy + mz * vz,
            py * mz - pz * my, pz * mx - px * mz, px * my - py * mx,
        )
        for k, term in enumerate(terms):
            part = term[:, 0:LANES]
            for n in range(LANES, width, LANES):
                part = part + term[:, n : n + LANES]
            part_ref[k, rows] = part

    raw = [jnp.sum(jnp.transpose(part_ref[k]), axis=0, keepdims=True) for k in range(MOMENTS)]
    w, rx, ry, rz, mx, my, mz, energy, ax, ay, az = raw
    table = rows_to_array(
        [
            w, rx + w * sx, ry + w * sy, rz + w * sz, mx, my, mz, energy,
            ax + (sy * mz - sz * my), ay + (sz * mx - sx * mz), az + (sx * my - sy * mx), slot,
        ],
        16, blocks,
    )
    for s in range(send_ref.shape[0]):
        for k in range(3):
            send_ref[s, :, k * blocks : (k + 1) * blocks] = table[4 * k : 4 * k + 4]


def outputs_kernel(
    groups, domains, halos,
    recv_ref, pos_ref, vel_ref, side_ref, cols_ref,
    table_hbm, kin_hbm, rad_hbm, table_ref, kin_ref, rad_ref, stats_ref, sems, table_sem,
):
    blocks, width = kin_ref.shape
    owned = halos // (groups * domains)
    group, domain = lax.axis_index("grp"), lax.axis_index("dom")

    near = []
    for offset in sorted({o % groups for o in (-1, 0, 1)}):
        source = lax.rem(group + offset, groups)
        for d in range(domains):
            part = recv_ref[d * groups + source]
            near.append(
                jnp.concatenate([part[:, k * blocks : (k + 1) * blocks] for k in range(3)], axis=0)
            )
    base = ((group * domains + domain) * owned).astype(jnp.float32)
    mine = cols_ref[1]
    own = lax.broadcasted_iota(jnp.int32, (owned, LANES), 0).astype(jnp.float32) + base
    want = jnp.concatenate([mine, own], axis=0)
    same = jnp.concatenate(
        [jnp.where(want == rows[MOMENTS : MOMENTS + 1], 1.0, 0.0).astype(jnp.bfloat16) for rows in near],
        axis=1,
    )
    values = jnp.concatenate(near, axis=1)
    values = jnp.concatenate([values, jnp.zeros((4, values.shape[1]), jnp.float32)], axis=0)
    top = values.astype(jnp.bfloat16)
    rest = values - top.astype(jnp.float32)
    mid = rest.astype(jnp.bfloat16)
    last = (rest - mid.astype(jnp.float32)).astype(jnp.bfloat16)
    sums = lax.dot_general(
        jnp.concatenate([top, mid, last], axis=0), same, (((1,), (1,)), ((), ())),
        preferred_element_type=jnp.float32,
    )
    sums = sums[0:16] + sums[16:32] + sums[32:48]

    heavy = jnp.maximum(sums[0:1], 1.0)
    mean = sums[0:8] / heavy
    cx, cy, cz, dx, dy, dz, energy = (mean[k : k + 1] for k in range(1, 8))
    spread = energy - (dx * dx + dy * dy + dz * dz)

    m = slice(0, blocks)
    side = side_ref[...]
    stats = rows_to_array(
        [
            cx[:, m] - side[1:2], cy[:, m] - side[2:3], cz[:, m] - side[3:4],
            dx[:, m], dy[:, m], dz[:, m], 1.0 / (3.0 * spread[:, m] + EPSILON),
        ],
        8, blocks,
    )
    stats_ref[...] = jnp.transpose(stats)

    whole = jnp.zeros((4, blocks), jnp.float32)
    for s in range(recv_ref.shape[0]):
        whole = whole + recv_ref[s, :, 0:blocks]
    total = jnp.sum(whole[0:1], axis=1, keepdims=True)
    o = slice(blocks, blocks + owned)
    share = sums[0:1, o] * float(halos) / total
    at = lax.broadcasted_iota(jnp.int32, (8, owned), 0)
    table_ref[0:8] = jnp.where(at == 0, share, jnp.where(at == 7, spread[:, o], mean[:, o]))
    cx, cy, cz, dx, dy, dz = (v[:, o] for v in (cx, cy, cz, dx, dy, dz))
    turn = rows_to_array([cy * dz - cz * dy, cz * dx - cx * dz, cx * dy - cy * dx], 8, owned)
    table_ref[8:11] = (sums[8:16, o] / heavy[:, o] - turn)[0:3]
    table_copy = pltpu.make_async_copy(table_ref, table_hbm, table_sem)
    table_copy.start()

    lane = lax.broadcasted_iota(jnp.int32, (8, width), 1).astype(jnp.float32)
    step = blocks // OUT_CHUNKS

    def leaving(c):
        part = pl.ds(pl.multiple_of(c * step, step), step)
        return (
            pltpu.make_async_copy(kin_ref.at[part], kin_hbm.at[part], sems.at[0, c]),
            pltpu.make_async_copy(rad_ref.at[part], rad_hbm.at[part], sems.at[1, c]),
        )

    @pl.loop(0, OUT_CHUNKS)
    def _(c):
        for r in range(0, step, 8):
            rows = pl.ds(pl.multiple_of(c * step + r, 8), 8)
            stat = stats_ref[rows]
            alive = lane < jnp.concatenate([cols_ref[0, rows]] * (width // LANES), axis=1)
            rx, ry, rz = (pos_ref[k, rows] - stat[:, k : k + 1] for k in range(3))
            ox, oy, oz = (vel_ref[k, rows] - stat[:, k + 3 : k + 4] for k in range(3))
            kinetic = (ox * ox + oy * oy + oz * oz) * stat[:, 6:7]
            kin_ref[rows] = jnp.where(alive, kinetic, 0.0)
            rad_ref[rows] = jnp.where(alive, rx * rx + ry * ry + rz * rz, 0.0)
        for copy in leaving(c):
            copy.start()

    for c in range(OUT_CHUNKS):
        for copy in leaving(c):
            copy.wait()
    table_copy.wait()


def local(positions, velocities, masses, block_halo, block_shift, block_live, block_count, home_slot):
    blocks, width = masses.shape
    halos = home_slot.shape[0]
    groups, domains = lax.axis_size("grp"), lax.axis_size("dom")
    devices = groups * domains
    anywhere = pl.BlockSpec(memory_space=pl.ANY)
    hbm = pl.BlockSpec(memory_space=pltpu.HBM)
    vmem = pl.BlockSpec(memory_space=pltpu.VMEM)
    held = functools.partial(pltpu.with_memory_space_constraint, memory_space=pltpu.HBM)
    send, pos, vel, side, cols = pl.pallas_call(
        moments_kernel,
        out_shape=(
            pltpu.VMEM((devices, 4, 3 * blocks), jnp.float32),
            pltpu.VMEM(positions.shape, jnp.float32),
            pltpu.VMEM(velocities.shape, jnp.float32),
            pltpu.VMEM((8, blocks), jnp.float32),
            pltpu.VMEM((2, blocks, LANES), jnp.float32),
        ),
        in_specs=[hbm] * 7 + [pl.BlockSpec(memory_space=pltpu.SMEM)],
        out_specs=(vmem,) * 5,
        scratch_shapes=[
            pltpu.VMEM((blocks, width), jnp.float32),
            pltpu.VMEM((MOMENTS, blocks, LANES), jnp.float32),
            pltpu.VMEM((1, blocks), jnp.int32),
            pltpu.VMEM((halos // LANES, LANES), jnp.int32),
            pltpu.VMEM((3, blocks), jnp.int32),
            pltpu.VMEM((1, blocks), jnp.int32),
            pltpu.SemaphoreType.DMA((3,)),
            pltpu.SemaphoreType.DMA((4,)),
        ],
        compiler_params=pltpu.CompilerParams(vmem_limit_bytes=16 * 1024 * 1024),
        name="moments",
    )(
        *map(
            held,
            (
                positions, velocities, masses, block_halo.reshape(1, blocks),
                home_slot.reshape(halos // LANES, LANES), block_shift, block_live.reshape(1, blocks),
            ),
        ),
        block_count,
    )
    recv = lax.all_to_all(send, AXES[::-1], 0, 0)
    table, kinetic, radial = pl.pallas_call(
        functools.partial(outputs_kernel, groups, domains, halos),
        out_shape=(
            jax.ShapeDtypeStruct((MOMENTS, halos // devices), jnp.float32),
            jax.ShapeDtypeStruct((blocks, width), jnp.float32),
            jax.ShapeDtypeStruct((blocks, width), jnp.float32),
        ),
        in_specs=[vmem] * 5,
        out_specs=(anywhere,) * 3,
        scratch_shapes=[
            pltpu.VMEM((MOMENTS, halos // devices), jnp.float32),
            pltpu.VMEM((blocks, width), jnp.float32),
            pltpu.VMEM((blocks, width), jnp.float32),
            pltpu.VMEM((blocks, 8), jnp.float32),
            pltpu.SemaphoreType.DMA((2, OUT_CHUNKS)),
            pltpu.SemaphoreType.DMA,
        ],
        compiler_params=pltpu.CompilerParams(vmem_limit_bytes=16 * 1024 * 1024),
        name="outputs",
    )(recv, pos, vel, side, cols)
    return table, kinetic, radial


def solution(mesh):
    return jax.shard_map(
        local,
        mesh=mesh,
        in_specs=(
            P(None, AXES, None), P(None, AXES, None), P(AXES, None), P(AXES),
            P(None, AXES), P(AXES), P(AXES), P(),
        ),
        out_specs=(P(None, AXES), P(AXES, None), P(AXES, None)),
        check_vma=False,
    )
```

```python
import functools

import jax
import jax.numpy as jnp
from jax import lax
from jax.experimental import pallas as pl
from jax.experimental.pallas import tpu as pltpu
from jax.sharding import PartitionSpec as P

EPSILON = 1e-06
LANES = 128
OUT_CHUNKS = 2
FLOPS = 1000000000
BYTES = 10000000
MOMENTS = 11
AXES = ("grp", "dom")


def rows_to_array(rows, count, width):
    at = lax.broadcasted_iota(jnp.int32, (count, width), 0)
    out = jnp.zeros((count, width), jnp.float32)
    for k, row in enumerate(rows):
        out = jnp.where(at == k, row, out)
    return out


def blocks_kernel(
    halo_hbm, home_hbm, shift_hbm, live_hbm, count_ref,
    side_ref, cols_ref, halo_ref, home_ref, shift_ref, live_ref, sems,
):
    blocks = side_ref.shape[1]
    copies = [
        pltpu.make_async_copy(src, dst, sems.at[k])
        for k, (src, dst) in enumerate(
            (
                (halo_hbm, halo_ref), (home_hbm, home_ref), (shift_hbm, shift_ref), (live_hbm, live_ref),
            )
        )
    ]
    for copy in copies:
        copy.start()
    for copy in copies:
        copy.wait()

    halo = halo_ref[...]
    low = lax.broadcasted_iota(jnp.int32, (LANES, blocks), 0) == halo % LANES
    picked = lax.dot_general(
        home_ref[...].astype(jnp.float32), low.astype(jnp.float32), (((1,), (0,)), ((), ())),
        precision=lax.Precision.HIGHEST, preferred_element_type=jnp.float32,
    )
    high = lax.broadcasted_iota(jnp.int32, picked.shape, 0) == halo // LANES
    slot = jnp.sum(jnp.where(high, picked, 0.0), axis=0, keepdims=True)

    at = lax.broadcasted_iota(jnp.int32, (1, blocks), 1)
    live = jnp.where(at < count_ref[0], live_ref[...], 0).astype(jnp.float32)
    shift = shift_ref[...].astype(jnp.float32)
    side_ref[...] = rows_to_array([live, shift[0:1], shift[1:2], shift[2:3], slot], 8, blocks)
    cols_ref[0] = jnp.transpose(jnp.broadcast_to(live, (LANES, blocks)))
    cols_ref[1] = jnp.transpose(jnp.broadcast_to(slot, (LANES, blocks)))


def moments_kernel(pos_ref, vel_ref, mass_ref, side_ref, cols_ref, send_ref, part_ref):
    blocks, width = mass_ref.shape
    side = side_ref[...]
    sx, sy, sz, slot = (side[k : k + 1] for k in range(1, 5))
    lane = lax.broadcasted_iota(jnp.int32, (8, width), 1).astype(jnp.float32)
    for r in range(0, blocks, 8):
        rows = slice(r, r + 8)
        edge = cols_ref[0, rows]
        edge = jnp.concatenate([edge] * (width // LANES), axis=1)
        weight = jnp.where(lane < edge, mass_ref[rows], 0.0)
        px, py, pz = (pos_ref[k, rows] for k in range(3))
        vx, vy, vz = (vel_ref[k, rows] for k in range(3))
        mx, my, mz = weight * vx, weight * vy, weight * vz
        terms = (
            weight, weight * px, weight * py, weight * pz, mx, my, mz,
            mx * vx + my * vy + mz * vz,
            py * mz - pz * my, pz * mx - px * mz, px * my - py * mx,
        )
        for k, term in enumerate(terms):
            part = term[:, 0:LANES]
            for n in range(LANES, width, LANES):
                part = part + term[:, n : n + LANES]
            part_ref[k, rows] = part

    raw = [jnp.sum(jnp.transpose(part_ref[k]), axis=0, keepdims=True) for k in range(MOMENTS)]
    w, rx, ry, rz, mx, my, mz, energy, ax, ay, az = raw
    table = rows_to_array(
        [
            w, rx + w * sx, ry + w * sy, rz + w * sz, mx, my, mz, energy,
            ax + (sy * mz - sz * my), ay + (sz * mx - sx * mz), az + (sx * my - sy * mx), slot,
        ],
        16, blocks,
    )
    for s in range(send_ref.shape[0]):
        for k in range(3):
            send_ref[s, :, k * blocks : (k + 1) * blocks] = table[4 * k : 4 * k + 4]


def outputs_kernel(
    groups, domains, halos,
    recv_ref, pos_ref, vel_ref, side_ref, cols_ref,
    table_hbm, kin_hbm, rad_hbm, table_ref, kin_ref, rad_ref, stats_ref, sems, table_sem,
):
    blocks, width = kin_ref.shape
    owned = halos // (groups * domains)
    group, domain = lax.axis_index("grp"), lax.axis_index("dom")

    near = []
    for offset in sorted({o % groups for o in (-1, 0, 1)}):
        source = lax.rem(group + offset, groups)
        for d in range(domains):
            part = recv_ref[d * groups + source]
            near.append(
                jnp.concatenate([part[:, k * blocks : (k + 1) * blocks] for k in range(3)], axis=0)
            )
    base = ((group * domains + domain) * owned).astype(jnp.float32)
    mine = cols_ref[1]
    own = lax.broadcasted_iota(jnp.int32, (owned, LANES), 0).astype(jnp.float32) + base
    want = jnp.concatenate([mine, own], axis=0)
    same = jnp.concatenate(
        [jnp.where(want == rows[MOMENTS : MOMENTS + 1], 1.0, 0.0).astype(jnp.bfloat16) for rows in near],
        axis=1,
    )
    values = jnp.concatenate(near, axis=1)
    values = jnp.concatenate([values, jnp.zeros((4, values.shape[1]), jnp.float32)], axis=0)
    top = values.astype(jnp.bfloat16)
    rest = values - top.astype(jnp.float32)
    mid = rest.astype(jnp.bfloat16)
    last = (rest - mid.astype(jnp.float32)).astype(jnp.bfloat16)
    sums = lax.dot_general(
        jnp.concatenate([top, mid, last], axis=0), same, (((1,), (1,)), ((), ())),
        preferred_element_type=jnp.float32,
    )
    sums = sums[0:16] + sums[16:32] + sums[32:48]

    heavy = jnp.maximum(sums[0:1], 1.0)
    mean = sums[0:8] / heavy
    cx, cy, cz, dx, dy, dz, energy = (mean[k : k + 1] for k in range(1, 8))
    spread = energy - (dx * dx + dy * dy + dz * dz)

    m = slice(0, blocks)
    side = side_ref[...]
    stats = rows_to_array(
        [
            cx[:, m] - side[1:2], cy[:, m] - side[2:3], cz[:, m] - side[3:4],
            dx[:, m], dy[:, m], dz[:, m], 1.0 / (3.0 * spread[:, m] + EPSILON),
        ],
        8, blocks,
    )
    stats_ref[...] = jnp.transpose(stats)

    whole = jnp.zeros((4, blocks), jnp.float32)
    for s in range(recv_ref.shape[0]):
        whole = whole + recv_ref[s, :, 0:blocks]
    total = jnp.sum(whole[0:1], axis=1, keepdims=True)
    o = slice(blocks, blocks + owned)
    share = sums[0:1, o] * float(halos) / total
    at = lax.broadcasted_iota(jnp.int32, (8, owned), 0)
    table_ref[0:8] = jnp.where(at == 0, share, jnp.where(at == 7, spread[:, o], mean[:, o]))
    cx, cy, cz, dx, dy, dz = (v[:, o] for v in (cx, cy, cz, dx, dy, dz))
    turn = rows_to_array([cy * dz - cz * dy, cz * dx - cx * dz, cx * dy - cy * dx], 8, owned)
    table_ref[8:11] = (sums[8:16, o] / heavy[:, o] - turn)[0:3]
    table_copy = pltpu.make_async_copy(table_ref, table_hbm, table_sem)
    table_copy.start()

    lane = lax.broadcasted_iota(jnp.int32, (8, width), 1).astype(jnp.float32)
    step = blocks // OUT_CHUNKS

    def leaving(c):
        part = pl.ds(pl.multiple_of(c * step, step), step)
        return (
            pltpu.make_async_copy(kin_ref.at[part], kin_hbm.at[part], sems.at[0, c]),
            pltpu.make_async_copy(rad_ref.at[part], rad_hbm.at[part], sems.at[1, c]),
        )

    @pl.loop(0, OUT_CHUNKS)
    def _(c):
        for r in range(0, step, 8):
            rows = pl.ds(pl.multiple_of(c * step + r, 8), 8)
            stat = stats_ref[rows]
            alive = lane < jnp.concatenate([cols_ref[0, rows]] * (width // LANES), axis=1)
            rx, ry, rz = (pos_ref[k, rows] - stat[:, k : k + 1] for k in range(3))
            ox, oy, oz = (vel_ref[k, rows] - stat[:, k + 3 : k + 4] for k in range(3))
            kinetic = (ox * ox + oy * oy + oz * oz) * stat[:, 6:7]
            kin_ref[rows] = jnp.where(alive, kinetic, 0.0)
            rad_ref[rows] = jnp.where(alive, rx * rx + ry * ry + rz * rz, 0.0)
        for copy in leaving(c):
            copy.start()

    for c in range(OUT_CHUNKS):
        for copy in leaving(c):
            copy.wait()
    table_copy.wait()


def local(positions, velocities, masses, block_halo, block_shift, block_live, block_count, home_slot):
    blocks, width = masses.shape
    halos = home_slot.shape[0]
    groups, domains = lax.axis_size("grp"), lax.axis_size("dom")
    devices = groups * domains
    anywhere = pl.BlockSpec(memory_space=pl.ANY)
    hbm = pl.BlockSpec(memory_space=pltpu.HBM)
    vmem = pl.BlockSpec(memory_space=pltpu.VMEM)
    smem = pl.BlockSpec(memory_space=pltpu.SMEM)
    held = functools.partial(pltpu.with_memory_space_constraint, memory_space=pltpu.HBM)
    side, cols = pl.pallas_call(
        blocks_kernel,
        out_shape=(
            pltpu.VMEM((8, blocks), jnp.float32),
            pltpu.VMEM((2, blocks, LANES), jnp.float32),
        ),
        in_specs=[hbm] * 4 + [smem],
        out_specs=(vmem,) * 2,
        scratch_shapes=[
            pltpu.VMEM((1, blocks), jnp.int32),
            pltpu.VMEM((halos // LANES, LANES), jnp.int32),
            pltpu.VMEM((3, blocks), jnp.int32),
            pltpu.VMEM((1, blocks), jnp.int32),
            pltpu.SemaphoreType.DMA((4,)),
        ],
        compiler_params=pltpu.CompilerParams(vmem_limit_bytes=1024 * 1024),
        cost_estimate=pl.CostEstimate(flops=FLOPS, bytes_accessed=BYTES, transcendentals=0),
        name="blocks",
    )(
        *map(
            held,
            (
                block_halo.reshape(1, blocks), home_slot.reshape(halos // LANES, LANES), block_shift,
                block_live.reshape(1, blocks),
            ),
        ),
        block_count,
    )
    send = pl.pallas_call(
        moments_kernel,
        out_shape=pltpu.VMEM((devices, 4, 3 * blocks), jnp.float32),
        in_specs=[vmem] * 5,
        out_specs=vmem,
        scratch_shapes=[pltpu.VMEM((MOMENTS, blocks, LANES), jnp.float32)],
        compiler_params=pltpu.CompilerParams(vmem_limit_bytes=8 * 1024 * 1024),
        name="moments",
    )(positions, velocities, masses, side, cols)
    recv = lax.all_to_all(send, AXES[::-1], 0, 0)
    table, kinetic, radial = pl.pallas_call(
        functools.partial(outputs_kernel, groups, domains, halos),
        out_shape=(
            jax.ShapeDtypeStruct((MOMENTS, halos // devices), jnp.float32),
            jax.ShapeDtypeStruct((blocks, width), jnp.float32),
            jax.ShapeDtypeStruct((blocks, width), jnp.float32),
        ),
        in_specs=[vmem] * 5,
        out_specs=(anywhere,) * 3,
        scratch_shapes=[
            pltpu.VMEM((MOMENTS, halos // devices), jnp.float32),
            pltpu.VMEM((blocks, width), jnp.float32),
            pltpu.VMEM((blocks, width), jnp.float32),
            pltpu.VMEM((blocks, 8), jnp.float32),
            pltpu.SemaphoreType.DMA((2, OUT_CHUNKS)),
            pltpu.SemaphoreType.DMA,
        ],
        compiler_params=pltpu.CompilerParams(vmem_limit_bytes=16 * 1024 * 1024),
        name="outputs",
    )(recv, positions, velocities, side, cols)
    return table, kinetic, radial


def solution(mesh):
    return jax.shard_map(
        local,
        mesh=mesh,
        in_specs=(
            P(None, AXES, None), P(None, AXES, None), P(AXES, None), P(AXES),
            P(None, AXES), P(AXES), P(AXES), P(),
        ),
        out_specs=(P(None, AXES), P(AXES, None), P(AXES, None)),
        check_vma=False,
    )
```

```python
import functools

import jax
import jax.numpy as jnp
from jax import lax
from jax.experimental import pallas as pl
from jax.experimental.pallas import tpu as pltpu
from jax.sharding import PartitionSpec as P

EPSILON = 1e-06
LANES = 128
OUT_CHUNKS = 2
MOMENTS = 11
AXES = ("grp", "dom")


def rows_to_array(rows, count, width):
    at = lax.broadcasted_iota(jnp.int32, (count, width), 0)
    out = jnp.zeros((count, width), jnp.float32)
    for k, row in enumerate(rows):
        out = jnp.where(at == k, row, out)
    return out


def moments_kernel(
    pos_hbm, vel_hbm, mass_hbm, halo_hbm, home_hbm, shift_hbm, live_hbm, count_ref,
    send_ref, pos_ref, vel_ref, side_ref, cols_ref, mass_ref, part_ref,
    halo_ref, home_ref, shift_ref, live_ref, sems, small_sems,
):
    blocks, width = mass_ref.shape
    small = [
        pltpu.make_async_copy(src, dst, small_sems.at[k])
        for k, (src, dst) in enumerate(
            (
                (halo_hbm, halo_ref), (home_hbm, home_ref), (shift_hbm, shift_ref), (live_hbm, live_ref),
            )
        )
    ]
    large = [
        pltpu.make_async_copy(src, dst, sems.at[k])
        for k, (src, dst) in enumerate(
            ((mass_hbm, mass_ref), (vel_hbm, vel_ref), (pos_hbm, pos_ref))
        )
    ]
    for copy in small + large:
        copy.start()

    for copy in small:
        copy.wait()

    halo = halo_ref[...]
    low = lax.broadcasted_iota(jnp.int32, (LANES, blocks), 0) == halo % LANES
    picked = lax.dot_general(
        home_ref[...].astype(jnp.float32), low.astype(jnp.float32), (((1,), (0,)), ((), ())),
        precision=lax.Precision.HIGHEST, preferred_element_type=jnp.float32,
    )
    high = lax.broadcasted_iota(jnp.int32, picked.shape, 0) == halo // LANES
    slot = jnp.sum(jnp.where(high, picked, 0.0), axis=0, keepdims=True)

    at = lax.broadcasted_iota(jnp.int32, (1, blocks), 1)
    live = jnp.where(at < count_ref[0], live_ref[...], 0).astype(jnp.float32)
    shift = shift_ref[...].astype(jnp.float32)
    sx, sy, sz = shift[0:1], shift[1:2], shift[2:3]
    side_ref[...] = rows_to_array([live, sx, sy, sz, slot], 8, blocks)
    cols_ref[0] = jnp.transpose(jnp.broadcast_to(live, (LANES, blocks)))
    cols_ref[1] = jnp.transpose(jnp.broadcast_to(slot, (LANES, blocks)))

    lane = lax.broadcasted_iota(jnp.int32, (8, width), 1).astype(jnp.float32)


    def keep(k, rows, term):
        part = term[:, 0:LANES]
        for n in range(LANES, width, LANES):
            part = part + term[:, n : n + LANES]
        part_ref[k, rows] = part

    def summed(k):
        return jnp.sum(jnp.transpose(part_ref[k]), axis=0, keepdims=True)

    raw = [None] * MOMENTS
    for copy in large[:2]:
        copy.wait()
    for r in range(0, blocks, 8):
        rows = slice(r, r + 8)
        edge = jnp.concatenate([cols_ref[0, rows]] * (width // LANES), axis=1)
        weight = jnp.where(lane < edge, mass_ref[rows], 0.0)
        vx, vy, vz = (vel_ref[k, rows] for k in range(3))
        mx, my, mz = weight * vx, weight * vy, weight * vz
        mass_ref[rows] = weight
        for k, term in ((0, weight), (4, mx), (5, my), (6, mz), (7, mx * vx + my * vy + mz * vz)):
            keep(k, rows, term)
    for k in (0, 4, 5, 6, 7):
        raw[k] = summed(k)
    large[2].wait()
    for r in range(0, blocks, 8):
        rows = slice(r, r + 8)
        weight = mass_ref[rows]
        vx, vy, vz = (vel_ref[k, rows] for k in range(3))
        qx, qy, qz = (weight * pos_ref[k, rows] for k in range(3))
        terms = (qx, qy, qz, qy * vz - qz * vy, qz * vx - qx * vz, qx * vy - qy * vx)
        for k, term in zip((1, 2, 3, 8, 9, 10), terms):
            keep(k, rows, term)
    for k in (1, 2, 3, 8, 9, 10):
        raw[k] = summed(k)

    w, rx, ry, rz, mx, my, mz, energy, ax, ay, az = raw
    table = rows_to_array(
        [
            w, rx + w * sx, ry + w * sy, rz + w * sz, mx, my, mz, energy,
            ax + (sy * mz - sz * my), ay + (sz * mx - sx * mz), az + (sx * my - sy * mx), slot,
        ],
        16, blocks,
    )
    for s in range(send_ref.shape[0]):
        for k in range(3):
            send_ref[s, :, k * blocks : (k + 1) * blocks] = table[4 * k : 4 * k + 4]


def outputs_kernel(
    groups, domains, halos,
    recv_ref, pos_ref, vel_ref, side_ref, cols_ref,
    table_hbm, kin_hbm, rad_hbm, table_ref, kin_ref, rad_ref, stats_ref, sems, table_sem,
):
    blocks, width = kin_ref.shape
    owned = halos // (groups * domains)
    group, domain = lax.axis_index("grp"), lax.axis_index("dom")

    near = []
    offsets = list(dict.fromkeys((0, groups - 1, 1 % groups)))
    for offset in offsets:
        source = lax.rem(group + offset, groups)
        for d in range(domains):
            part = recv_ref[d * groups + source]
            near.append(
                jnp.concatenate([part[:, k * blocks : (k + 1) * blocks] for k in range(3)], axis=0)
            )
    feeders = domains * len({0, groups - 1})
    base = ((group * domains + domain) * owned).astype(jnp.float32)
    own = lax.broadcasted_iota(jnp.int32, (owned, LANES), 0).astype(jnp.float32) + base
    values = jnp.concatenate(near, axis=1)
    values = jnp.concatenate([values, jnp.zeros((4, values.shape[1]), jnp.float32)], axis=0)
    top = values.astype(jnp.bfloat16)
    rest = values - top.astype(jnp.float32)
    mid = rest.astype(jnp.bfloat16)
    last = (rest - mid.astype(jnp.float32)).astype(jnp.bfloat16)
    terms = jnp.concatenate([top, mid, last], axis=0)

    def taken(want, sources):
        same = jnp.concatenate(
            [
                jnp.where(want == rows[MOMENTS : MOMENTS + 1], 1.0, 0.0).astype(jnp.bfloat16)
                for rows in near[:sources]
            ],
            axis=1,
        )
        out = lax.dot_general(
            terms[:, 0 : sources * blocks], same, (((1,), (1,)), ((), ())),
            preferred_element_type=jnp.float32,
        )
        return out[0:16] + out[16:32] + out[32:48]

    sums = jnp.concatenate([taken(cols_ref[1], len(near)), taken(own, feeders)], axis=1)

    heavy = jnp.maximum(sums[0:1], 1.0)
    mean = sums[0:8] / heavy
    cx, cy, cz, dx, dy, dz, energy = (mean[k : k + 1] for k in range(1, 8))
    spread = energy - (dx * dx + dy * dy + dz * dz)

    m = slice(0, blocks)
    side = side_ref[...]
    stats = rows_to_array(
        [
            cx[:, m] - side[1:2], cy[:, m] - side[2:3], cz[:, m] - side[3:4],
            dx[:, m], dy[:, m], dz[:, m], 1.0 / (3.0 * spread[:, m] + EPSILON),
        ],
        8, blocks,
    )
    stats_ref[...] = jnp.transpose(stats)

    lane = lax.broadcasted_iota(jnp.int32, (8, width), 1).astype(jnp.float32)
    step = blocks // OUT_CHUNKS

    def leaving(c):
        part = slice(c * step, (c + 1) * step)
        return (
            pltpu.make_async_copy(kin_ref.at[part], kin_hbm.at[part], sems.at[0, c]),
            pltpu.make_async_copy(rad_ref.at[part], rad_hbm.at[part], sems.at[1, c]),
        )

    for c in range(OUT_CHUNKS):
        for r in range(0, step, 8):
            rows = slice(c * step + r, c * step + r + 8)
            stat = stats_ref[rows]
            alive = lane < jnp.concatenate([cols_ref[0, rows]] * (width // LANES), axis=1)
            rx, ry, rz = (pos_ref[k, rows] - stat[:, k : k + 1] for k in range(3))
            ox, oy, oz = (vel_ref[k, rows] - stat[:, k + 3 : k + 4] for k in range(3))
            kinetic = (ox * ox + oy * oy + oz * oz) * stat[:, 6:7]
            kin_ref[rows] = jnp.where(alive, kinetic, 0.0)
            rad_ref[rows] = jnp.where(alive, rx * rx + ry * ry + rz * rz, 0.0)
        for copy in leaving(c):
            copy.start()

    whole = jnp.zeros((4, blocks), jnp.float32)
    for s in range(recv_ref.shape[0]):
        whole = whole + recv_ref[s, :, 0:blocks]
    total = jnp.sum(whole[0:1], axis=1, keepdims=True)
    o = slice(blocks, blocks + owned)
    share = sums[0:1, o] * float(halos) / total
    at = lax.broadcasted_iota(jnp.int32, (8, owned), 0)
    table_ref[0:8] = jnp.where(at == 0, share, jnp.where(at == 7, spread[:, o], mean[:, o]))
    cx, cy, cz, dx, dy, dz = (v[:, o] for v in (cx, cy, cz, dx, dy, dz))
    turn = rows_to_array([cy * dz - cz * dy, cz * dx - cx * dz, cx * dy - cy * dx], 8, owned)
    table_ref[8:11] = (sums[8:16, o] / heavy[:, o] - turn)[0:3]
    table_copy = pltpu.make_async_copy(table_ref, table_hbm, table_sem)
    table_copy.start()

    for c in range(OUT_CHUNKS):
        for copy in leaving(c):
            copy.wait()
    table_copy.wait()


def local(positions, velocities, masses, block_halo, block_shift, block_live, block_count, home_slot):
    blocks, width = masses.shape
    halos = home_slot.shape[0]
    groups, domains = lax.axis_size("grp"), lax.axis_size("dom")
    devices = groups * domains
    anywhere = pl.BlockSpec(memory_space=pl.ANY)
    hbm = pl.BlockSpec(memory_space=pltpu.HBM)
    vmem = pl.BlockSpec(memory_space=pltpu.VMEM)
    held = functools.partial(pltpu.with_memory_space_constraint, memory_space=pltpu.HBM)
    send, pos, vel, side, cols = pl.pallas_call(
        moments_kernel,
        out_shape=(
            pltpu.VMEM((devices, 4, 3 * blocks), jnp.float32),
            pltpu.VMEM(positions.shape, jnp.float32),
            pltpu.VMEM(velocities.shape, jnp.float32),
            pltpu.VMEM((8, blocks), jnp.float32),
            pltpu.VMEM((2, blocks, LANES), jnp.float32),
        ),
        in_specs=[hbm] * 7 + [pl.BlockSpec(memory_space=pltpu.SMEM)],
        out_specs=(vmem,) * 5,
        scratch_shapes=[
            pltpu.VMEM((blocks, width), jnp.float32),
            pltpu.VMEM((MOMENTS, blocks, LANES), jnp.float32),
            pltpu.VMEM((1, blocks), jnp.int32),
            pltpu.VMEM((halos // LANES, LANES), jnp.int32),
            pltpu.VMEM((3, blocks), jnp.int32),
            pltpu.VMEM((1, blocks), jnp.int32),
            pltpu.SemaphoreType.DMA((3,)),
            pltpu.SemaphoreType.DMA((4,)),
        ],
        compiler_params=pltpu.CompilerParams(vmem_limit_bytes=16 * 1024 * 1024),
        name="moments",
    )(
        *map(
            held,
            (
                positions, velocities, masses, block_halo.reshape(1, blocks),
                home_slot.reshape(halos // LANES, LANES), block_shift, block_live.reshape(1, blocks),
            ),
        ),
        block_count,
    )
    recv = lax.all_to_all(send, AXES[::-1], 0, 0)
    table, kinetic, radial = pl.pallas_call(
        functools.partial(outputs_kernel, groups, domains, halos),
        out_shape=(
            jax.ShapeDtypeStruct((MOMENTS, halos // devices), jnp.float32),
            jax.ShapeDtypeStruct((blocks, width), jnp.float32),
            jax.ShapeDtypeStruct((blocks, width), jnp.float32),
        ),
        in_specs=[vmem] * 5,
        out_specs=(anywhere,) * 3,
        scratch_shapes=[
            pltpu.VMEM((MOMENTS, halos // devices), jnp.float32),
            pltpu.VMEM((blocks, width), jnp.float32),
            pltpu.VMEM((blocks, width), jnp.float32),
            pltpu.VMEM((blocks, 8), jnp.float32),
            pltpu.SemaphoreType.DMA((2, OUT_CHUNKS)),
            pltpu.SemaphoreType.DMA,
        ],
        compiler_params=pltpu.CompilerParams(vmem_limit_bytes=16 * 1024 * 1024),
        name="outputs",
    )(recv, pos, vel, side, cols)
    return table, kinetic, radial


def solution(mesh):
    return jax.shard_map(
        local,
        mesh=mesh,
        in_specs=(
            P(None, AXES, None), P(None, AXES, None), P(AXES, None), P(AXES),
            P(None, AXES), P(AXES), P(AXES), P(),
        ),
        out_specs=(P(None, AXES), P(AXES, None), P(AXES, None)),
        check_vma=False,
    )
```

```python
import functools

import jax
import jax.numpy as jnp
from jax import lax
from jax.experimental import pallas as pl
from jax.experimental.pallas import tpu as pltpu
from jax.sharding import PartitionSpec as P

EPSILON = 1e-06
LANES = 128
OUT_CHUNKS = 4
MOMENTS = 11
AXES = ("grp", "dom")


def rows_to_array(rows, count, width):
    at = lax.broadcasted_iota(jnp.int32, (count, width), 0)
    out = jnp.zeros((count, width), jnp.float32)
    for k, row in enumerate(rows):
        out = jnp.where(at == k, row, out)
    return out


def moments_kernel(
    pos_hbm, vel_hbm, mass_hbm, halo_hbm, home_hbm, shift_hbm, live_hbm, count_ref,
    send_ref, pos_ref, vel_ref, side_ref, cols_ref, mass_ref, part_ref,
    halo_ref, home_ref, shift_ref, live_ref, sems, small_sems,
):
    blocks, width = mass_ref.shape
    small = [
        pltpu.make_async_copy(src, dst, small_sems.at[k])
        for k, (src, dst) in enumerate(
            (
                (halo_hbm, halo_ref), (home_hbm, home_ref), (shift_hbm, shift_ref), (live_hbm, live_ref),
            )
        )
    ]
    large = [
        pltpu.make_async_copy(src, dst, sems.at[k])
        for k, (src, dst) in enumerate(
            ((mass_hbm, mass_ref), (vel_hbm, vel_ref), (pos_hbm, pos_ref))
        )
    ]
    for copy in small + large:
        copy.start()

    for copy in small:
        copy.wait()

    halo = halo_ref[...]
    low = lax.broadcasted_iota(jnp.int32, (LANES, blocks), 0) == halo % LANES
    picked = lax.dot_general(
        home_ref[...].astype(jnp.float32), low.astype(jnp.float32), (((1,), (0,)), ((), ())),
        precision=lax.Precision.HIGHEST, preferred_element_type=jnp.float32,
    )
    high = lax.broadcasted_iota(jnp.int32, picked.shape, 0) == halo // LANES
    slot = jnp.sum(jnp.where(high, picked, 0.0), axis=0, keepdims=True)

    at = lax.broadcasted_iota(jnp.int32, (1, blocks), 1)
    live = jnp.where(at < count_ref[0], live_ref[...], 0).astype(jnp.float32)
    shift = shift_ref[...].astype(jnp.float32)
    sx, sy, sz = shift[0:1], shift[1:2], shift[2:3]
    side_ref[...] = rows_to_array([live, sx, sy, sz, slot], 8, blocks)
    cols_ref[0] = jnp.transpose(jnp.broadcast_to(live, (LANES, blocks)))
    cols_ref[1] = jnp.transpose(jnp.broadcast_to(slot, (LANES, blocks)))

    lane = lax.broadcasted_iota(jnp.int32, (8, width), 1).astype(jnp.float32)


    def keep(k, rows, term):
        part = term[:, 0:LANES]
        for n in range(LANES, width, LANES):
            part = part + term[:, n : n + LANES]
        part_ref[k, rows] = part

    def summed(k):
        return jnp.sum(jnp.transpose(part_ref[k]), axis=0, keepdims=True)

    raw = [None] * MOMENTS
    for copy in large[:2]:
        copy.wait()
    for r in range(0, blocks, 8):
        rows = slice(r, r + 8)
        edge = jnp.concatenate([cols_ref[0, rows]] * (width // LANES), axis=1)
        weight = jnp.where(lane < edge, mass_ref[rows], 0.0)
        vx, vy, vz = (vel_ref[k, rows] for k in range(3))
        mx, my, mz = weight * vx, weight * vy, weight * vz
        mass_ref[rows] = weight
        for k, term in ((0, weight), (4, mx), (5, my), (6, mz), (7, mx * vx + my * vy + mz * vz)):
            keep(k, rows, term)
    for k in (0, 4, 5, 6, 7):
        raw[k] = summed(k)
    large[2].wait()
    for r in range(0, blocks, 8):
        rows = slice(r, r + 8)
        weight = mass_ref[rows]
        vx, vy, vz = (vel_ref[k, rows] for k in range(3))
        qx, qy, qz = (weight * pos_ref[k, rows] for k in range(3))
        terms = (qx, qy, qz, qy * vz - qz * vy, qz * vx - qx * vz, qx * vy - qy * vx)
        for k, term in zip((1, 2, 3, 8, 9, 10), terms):
            keep(k, rows, term)
    for k in (1, 2, 3, 8, 9, 10):
        raw[k] = summed(k)

    w, rx, ry, rz, mx, my, mz, energy, ax, ay, az = raw
    table = rows_to_array(
        [
            w, rx + w * sx, ry + w * sy, rz + w * sz, mx, my, mz, energy,
            ax + (sy * mz - sz * my), ay + (sz * mx - sx * mz), az + (sx * my - sy * mx), slot,
        ],
        16, blocks,
    )
    for s in range(send_ref.shape[0]):
        for k in range(3):
            send_ref[s, :, k * blocks : (k + 1) * blocks] = table[4 * k : 4 * k + 4]


def outputs_kernel(
    groups, domains, halos,
    recv_ref, pos_ref, vel_ref, side_ref, cols_ref,
    table_hbm, kin_hbm, rad_hbm, table_ref, kin_ref, rad_ref, stats_ref, sems, table_sem,
):
    blocks, width = kin_ref.shape
    owned = halos // (groups * domains)
    group, domain = lax.axis_index("grp"), lax.axis_index("dom")

    near = []
    offsets = list(dict.fromkeys((0, groups - 1, 1 % groups)))
    for offset in offsets:
        source = lax.rem(group + offset, groups)
        for d in range(domains):
            part = recv_ref[d * groups + source]
            near.append(
                jnp.concatenate([part[:, k * blocks : (k + 1) * blocks] for k in range(3)], axis=0)
            )
    feeders = domains * len({0, groups - 1})
    base = ((group * domains + domain) * owned).astype(jnp.float32)
    own = lax.broadcasted_iota(jnp.int32, (owned, LANES), 0).astype(jnp.float32) + base
    values = jnp.concatenate(near, axis=1)
    values = jnp.concatenate([values, jnp.zeros((4, values.shape[1]), jnp.float32)], axis=0)
    top = values.astype(jnp.bfloat16)
    rest = values - top.astype(jnp.float32)
    mid = rest.astype(jnp.bfloat16)
    last = (rest - mid.astype(jnp.float32)).astype(jnp.bfloat16)
    terms = jnp.concatenate([top, mid, last], axis=0)

    def taken(want, sources):
        same = jnp.concatenate(
            [
                jnp.where(want == rows[MOMENTS : MOMENTS + 1], 1.0, 0.0).astype(jnp.bfloat16)
                for rows in near[:sources]
            ],
            axis=1,
        )
        out = lax.dot_general(
            terms[:, 0 : sources * blocks], same, (((1,), (1,)), ((), ())),
            preferred_element_type=jnp.float32,
        )
        return out[0:16] + out[16:32] + out[32:48]

    def means(sums):
        heavy = jnp.maximum(sums[0:1], 1.0)
        mean = sums[0:8] / heavy
        cx, cy, cz, dx, dy, dz, energy = (mean[k : k + 1] for k in range(1, 8))
        spread = energy - (dx * dx + dy * dy + dz * dz)
        return heavy, mean, (cx, cy, cz), (dx, dy, dz), spread

    _, _, centre, drift, spread = means(taken(cols_ref[1], len(near)))
    side = side_ref[...]
    stats = rows_to_array(
        [
            *(centre[k] - side[k + 1 : k + 2] for k in range(3)),
            *drift, 1.0 / (3.0 * spread + EPSILON),
        ],
        8, blocks,
    )
    stats_ref[...] = jnp.transpose(stats)

    lane = lax.broadcasted_iota(jnp.int32, (8, width), 1).astype(jnp.float32)
    step = blocks // OUT_CHUNKS

    def leaving(c):
        part = slice(c * step, (c + 1) * step)
        return (
            pltpu.make_async_copy(kin_ref.at[part], kin_hbm.at[part], sems.at[0, c]),
            pltpu.make_async_copy(rad_ref.at[part], rad_hbm.at[part], sems.at[1, c]),
        )

    for c in range(OUT_CHUNKS):
        for r in range(0, step, 8):
            rows = slice(c * step + r, c * step + r + 8)
            stat = stats_ref[rows]
            alive = lane < jnp.concatenate([cols_ref[0, rows]] * (width // LANES), axis=1)
            rx, ry, rz = (pos_ref[k, rows] - stat[:, k : k + 1] for k in range(3))
            ox, oy, oz = (vel_ref[k, rows] - stat[:, k + 3 : k + 4] for k in range(3))
            kinetic = (ox * ox + oy * oy + oz * oz) * stat[:, 6:7]
            kin_ref[rows] = jnp.where(alive, kinetic, 0.0)
            rad_ref[rows] = jnp.where(alive, rx * rx + ry * ry + rz * rz, 0.0)
        for k, copy in enumerate(leaving(c)):
            copy.start(priority=k)

    whole = jnp.zeros((4, blocks), jnp.float32)
    for s in range(recv_ref.shape[0]):
        whole = whole + recv_ref[s, :, 0:blocks]
    total = jnp.sum(whole[0:1], axis=1, keepdims=True)
    sums = taken(own, feeders)
    heavy, mean, (cx, cy, cz), (dx, dy, dz), spread = means(sums)
    share = sums[0:1] * float(halos) / total
    at = lax.broadcasted_iota(jnp.int32, (8, owned), 0)
    table_ref[0:8] = jnp.where(at == 0, share, jnp.where(at == 7, spread, mean))
    turn = rows_to_array([cy * dz - cz * dy, cz * dx - cx * dz, cx * dy - cy * dx], 8, owned)
    table_ref[8:11] = (sums[8:16] / heavy - turn)[0:3]
    table_copy = pltpu.make_async_copy(table_ref, table_hbm, table_sem)
    table_copy.start()

    for c in range(OUT_CHUNKS):
        for copy in leaving(c):
            copy.wait()
    table_copy.wait()


def local(positions, velocities, masses, block_halo, block_shift, block_live, block_count, home_slot):
    blocks, width = masses.shape
    halos = home_slot.shape[0]
    groups, domains = lax.axis_size("grp"), lax.axis_size("dom")
    devices = groups * domains
    anywhere = pl.BlockSpec(memory_space=pl.ANY)
    hbm = pl.BlockSpec(memory_space=pltpu.HBM)
    vmem = pl.BlockSpec(memory_space=pltpu.VMEM)
    held = functools.partial(pltpu.with_memory_space_constraint, memory_space=pltpu.HBM)
    send, pos, vel, side, cols = pl.pallas_call(
        moments_kernel,
        out_shape=(
            pltpu.VMEM((devices, 4, 3 * blocks), jnp.float32),
            pltpu.VMEM(positions.shape, jnp.float32),
            pltpu.VMEM(velocities.shape, jnp.float32),
            pltpu.VMEM((8, blocks), jnp.float32),
            pltpu.VMEM((2, blocks, LANES), jnp.float32),
        ),
        in_specs=[hbm] * 7 + [pl.BlockSpec(memory_space=pltpu.SMEM)],
        out_specs=(vmem,) * 5,
        scratch_shapes=[
            pltpu.VMEM((blocks, width), jnp.float32),
            pltpu.VMEM((MOMENTS, blocks, LANES), jnp.float32),
            pltpu.VMEM((1, blocks), jnp.int32),
            pltpu.VMEM((halos // LANES, LANES), jnp.int32),
            pltpu.VMEM((3, blocks), jnp.int32),
            pltpu.VMEM((1, blocks), jnp.int32),
            pltpu.SemaphoreType.DMA((3,)),
            pltpu.SemaphoreType.DMA((4,)),
        ],
        compiler_params=pltpu.CompilerParams(vmem_limit_bytes=16 * 1024 * 1024),
        name="moments",
    )(
        *map(
            held,
            (
                positions, velocities, masses, block_halo.reshape(1, blocks),
                home_slot.reshape(halos // LANES, LANES), block_shift, block_live.reshape(1, blocks),
            ),
        ),
        block_count,
    )
    recv = lax.all_to_all(send, AXES[::-1], 0, 0)
    table, kinetic, radial = pl.pallas_call(
        functools.partial(outputs_kernel, groups, domains, halos),
        out_shape=(
            jax.ShapeDtypeStruct((MOMENTS, halos // devices), jnp.float32),
            jax.ShapeDtypeStruct((blocks, width), jnp.float32),
            jax.ShapeDtypeStruct((blocks, width), jnp.float32),
        ),
        in_specs=[vmem] * 5,
        out_specs=(anywhere,) * 3,
        scratch_shapes=[
            pltpu.VMEM((MOMENTS, halos // devices), jnp.float32),
            pltpu.VMEM((blocks, width), jnp.float32),
            pltpu.VMEM((blocks, width), jnp.float32),
            pltpu.VMEM((blocks, 8), jnp.float32),
            pltpu.SemaphoreType.DMA((2, OUT_CHUNKS)),
            pltpu.SemaphoreType.DMA,
        ],
        compiler_params=pltpu.CompilerParams(vmem_limit_bytes=16 * 1024 * 1024),
        name="outputs",
    )(recv, pos, vel, side, cols)
    return table, kinetic, radial


def solution(mesh):
    return jax.shard_map(
        local,
        mesh=mesh,
        in_specs=(
            P(None, AXES, None), P(None, AXES, None), P(AXES, None), P(AXES),
            P(None, AXES), P(AXES), P(AXES), P(),
        ),
        out_specs=(P(None, AXES), P(AXES, None), P(AXES, None)),
        check_vma=False,
    )
```

```python
import functools

import jax
import jax.numpy as jnp
from jax import lax
from jax.experimental import pallas as pl
from jax.experimental.pallas import tpu as pltpu
from jax.sharding import PartitionSpec as P

EPSILON = 1e-06
LANES = 128
OUT_CHUNKS = 2
MOMENTS = 11
AXES = ("grp", "dom")


def rows_to_array(rows, count, width):
    at = lax.broadcasted_iota(jnp.int32, (count, width), 0)
    out = jnp.zeros((count, width), jnp.float32)
    for k, row in enumerate(rows):
        out = jnp.where(at == k, row, out)
    return out


def moments_kernel(
    pos_hbm, vel_hbm, mass_hbm, halo_hbm, home_hbm, shift_hbm, live_hbm, count_ref,
    send_ref, pos_ref, vel_ref, side_ref, cols_ref, mass_ref, part_ref,
    halo_ref, home_ref, shift_ref, live_ref, sems, small_sems,
):
    blocks, width = mass_ref.shape
    small = [
        pltpu.make_async_copy(src, dst, small_sems.at[k])
        for k, (src, dst) in enumerate(
            (
                (halo_hbm, halo_ref), (home_hbm, home_ref), (shift_hbm, shift_ref), (live_hbm, live_ref),
            )
        )
    ]
    large = [
        pltpu.make_async_copy(src, dst, sems.at[k])
        for k, (src, dst) in enumerate(
            ((mass_hbm, mass_ref), (vel_hbm, vel_ref), (pos_hbm, pos_ref))
        )
    ]
    for copy in small + large[:2]:
        copy.start()
    large[2].start(priority=1)

    for copy in small:
        copy.wait()

    halo = halo_ref[...]
    low = lax.broadcasted_iota(jnp.int32, (LANES, blocks), 0) == halo % LANES
    picked = lax.dot_general(
        home_ref[...].astype(jnp.float32), low.astype(jnp.float32), (((1,), (0,)), ((), ())),
        precision=lax.Precision.HIGHEST, preferred_element_type=jnp.float32,
    )
    high = lax.broadcasted_iota(jnp.int32, picked.shape, 0) == halo // LANES
    slot = jnp.sum(jnp.where(high, picked, 0.0), axis=0, keepdims=True)

    at = lax.broadcasted_iota(jnp.int32, (1, blocks), 1)
    live = jnp.where(at < count_ref[0], live_ref[...], 0).astype(jnp.float32)
    shift = shift_ref[...].astype(jnp.float32)
    sx, sy, sz = shift[0:1], shift[1:2], shift[2:3]
    side_ref[...] = rows_to_array([live, sx, sy, sz, slot], 8, blocks)
    cols_ref[0] = jnp.transpose(jnp.broadcast_to(live, (LANES, blocks)))
    cols_ref[1] = jnp.transpose(jnp.broadcast_to(slot, (LANES, blocks)))

    lane = lax.broadcasted_iota(jnp.int32, (8, width), 1).astype(jnp.float32)


    def keep(k, rows, term):
        part = term[:, 0:LANES]
        for n in range(LANES, width, LANES):
            part = part + term[:, n : n + LANES]
        part_ref[k, rows] = part

    def summed(k):
        return jnp.sum(jnp.transpose(part_ref[k]), axis=0, keepdims=True)

    raw = [None] * MOMENTS
    for copy in large[:2]:
        copy.wait()
    for r in range(0, blocks, 8):
        rows = slice(r, r + 8)
        edge = jnp.concatenate([cols_ref[0, rows]] * (width // LANES), axis=1)
        weight = jnp.where(lane < edge, mass_ref[rows], 0.0)
        vx, vy, vz = (vel_ref[k, rows] for k in range(3))
        mx, my, mz = weight * vx, weight * vy, weight * vz
        mass_ref[rows] = weight
        for k, term in ((0, weight), (4, mx), (5, my), (6, mz), (7, mx * vx + my * vy + mz * vz)):
            keep(k, rows, term)
    for k in (0, 4, 5, 6, 7):
        raw[k] = summed(k)
    large[2].wait()
    for r in range(0, blocks, 8):
        rows = slice(r, r + 8)
        weight = mass_ref[rows]
        vx, vy, vz = (vel_ref[k, rows] for k in range(3))
        qx, qy, qz = (weight * pos_ref[k, rows] for k in range(3))
        terms = (qx, qy, qz, qy * vz - qz * vy, qz * vx - qx * vz, qx * vy - qy * vx)
        for k, term in zip((1, 2, 3, 8, 9, 10), terms):
            keep(k, rows, term)
    for k in (1, 2, 3, 8, 9, 10):
        raw[k] = summed(k)

    w, rx, ry, rz, mx, my, mz, energy, ax, ay, az = raw
    table = rows_to_array(
        [
            w, rx + w * sx, ry + w * sy, rz + w * sz, mx, my, mz, energy,
            ax + (sy * mz - sz * my), ay + (sz * mx - sx * mz), az + (sx * my - sy * mx), slot,
        ],
        16, blocks,
    )
    for s in range(send_ref.shape[0]):
        for k in range(3):
            send_ref[s, :, k * blocks : (k + 1) * blocks] = table[4 * k : 4 * k + 4]


def outputs_kernel(
    groups, domains, halos,
    recv_ref, pos_ref, vel_ref, side_ref, cols_ref,
    table_hbm, kin_hbm, rad_hbm, table_ref, kin_ref, rad_ref, stats_ref, sems, table_sem,
):
    blocks, width = kin_ref.shape
    owned = halos // (groups * domains)
    group, domain = lax.axis_index("grp"), lax.axis_index("dom")

    near = []
    offsets = list(dict.fromkeys((0, groups - 1, 1 % groups)))
    for offset in offsets:
        source = lax.rem(group + offset, groups)
        for d in range(domains):
            part = recv_ref[d * groups + source]
            near.append(
                jnp.concatenate([part[:, k * blocks : (k + 1) * blocks] for k in range(3)], axis=0)
            )
    feeders = domains * len({0, groups - 1})
    base = ((group * domains + domain) * owned).astype(jnp.float32)
    own = lax.broadcasted_iota(jnp.int32, (owned, LANES), 0).astype(jnp.float32) + base
    values = jnp.concatenate(near, axis=1)
    values = jnp.concatenate([values, jnp.zeros((4, values.shape[1]), jnp.float32)], axis=0)
    top = values.astype(jnp.bfloat16)
    rest = values - top.astype(jnp.float32)
    mid = rest.astype(jnp.bfloat16)
    last = (rest - mid.astype(jnp.float32)).astype(jnp.bfloat16)
    terms = jnp.concatenate([top, mid, last], axis=0)

    def taken(want, sources):
        same = jnp.concatenate(
            [
                jnp.where(want == rows[MOMENTS : MOMENTS + 1], 1.0, 0.0).astype(jnp.bfloat16)
                for rows in near[:sources]
            ],
            axis=1,
        )
        out = lax.dot_general(
            terms[:, 0 : sources * blocks], same, (((1,), (1,)), ((), ())),
            preferred_element_type=jnp.float32,
        )
        return out[0:16] + out[16:32] + out[32:48]

    def means(sums):
        heavy = jnp.maximum(sums[0:1], 1.0)
        mean = sums[0:8] / heavy
        cx, cy, cz, dx, dy, dz, energy = (mean[k : k + 1] for k in range(1, 8))
        spread = energy - (dx * dx + dy * dy + dz * dz)
        return heavy, mean, (cx, cy, cz), (dx, dy, dz), spread

    _, _, centre, drift, spread = means(taken(cols_ref[1], len(near)))
    side = side_ref[...]
    stats = rows_to_array(
        [
            *(centre[k] - side[k + 1 : k + 2] for k in range(3)),
            *drift, 1.0 / (3.0 * spread + EPSILON),
        ],
        8, blocks,
    )
    stats_ref[...] = jnp.transpose(stats)

    lane = lax.broadcasted_iota(jnp.int32, (8, width), 1).astype(jnp.float32)
    step = blocks // OUT_CHUNKS

    def leaving(c):
        part = slice(c * step, (c + 1) * step)
        return (
            pltpu.make_async_copy(kin_ref.at[part], kin_hbm.at[part], sems.at[0, c]),
            pltpu.make_async_copy(rad_ref.at[part], rad_hbm.at[part], sems.at[1, c]),
        )

    for c in range(OUT_CHUNKS):
        for r in range(0, step, 8):
            rows = slice(c * step + r, c * step + r + 8)
            stat = stats_ref[rows]
            alive = lane < jnp.concatenate([cols_ref[0, rows]] * (width // LANES), axis=1)
            rx, ry, rz = (pos_ref[k, rows] - stat[:, k : k + 1] for k in range(3))
            ox, oy, oz = (vel_ref[k, rows] - stat[:, k + 3 : k + 4] for k in range(3))
            kinetic = (ox * ox + oy * oy + oz * oz) * stat[:, 6:7]
            kin_ref[rows] = jnp.where(alive, kinetic, 0.0)
            rad_ref[rows] = jnp.where(alive, rx * rx + ry * ry + rz * rz, 0.0)
        for k, copy in enumerate(leaving(c)):
            copy.start(priority=k)

    whole = jnp.zeros((4, blocks), jnp.float32)
    for s in range(recv_ref.shape[0]):
        whole = whole + recv_ref[s, :, 0:blocks]
    total = jnp.sum(whole[0:1], axis=1, keepdims=True)
    sums = taken(own, feeders)
    heavy, mean, (cx, cy, cz), (dx, dy, dz), spread = means(sums)
    share = sums[0:1] * float(halos) / total
    at = lax.broadcasted_iota(jnp.int32, (8, owned), 0)
    table_ref[0:8] = jnp.where(at == 0, share, jnp.where(at == 7, spread, mean))
    turn = rows_to_array([cy * dz - cz * dy, cz * dx - cx * dz, cx * dy - cy * dx], 8, owned)
    table_ref[8:11] = (sums[8:16] / heavy - turn)[0:3]
    table_copy = pltpu.make_async_copy(table_ref, table_hbm, table_sem)
    table_copy.start()

    for c in range(OUT_CHUNKS):
        for copy in leaving(c):
            copy.wait()
    table_copy.wait()


def local(positions, velocities, masses, block_halo, block_shift, block_live, block_count, home_slot):
    blocks, width = masses.shape
    halos = home_slot.shape[0]
    groups, domains = lax.axis_size("grp"), lax.axis_size("dom")
    devices = groups * domains
    anywhere = pl.BlockSpec(memory_space=pl.ANY)
    hbm = pl.BlockSpec(memory_space=pltpu.HBM)
    vmem = pl.BlockSpec(memory_space=pltpu.VMEM)
    held = functools.partial(pltpu.with_memory_space_constraint, memory_space=pltpu.HBM)
    send, pos, vel, side, cols = pl.pallas_call(
        moments_kernel,
        out_shape=(
            pltpu.VMEM((devices, 4, 3 * blocks), jnp.float32),
            pltpu.VMEM(positions.shape, jnp.float32),
            pltpu.VMEM(velocities.shape, jnp.float32),
            pltpu.VMEM((8, blocks), jnp.float32),
            pltpu.VMEM((2, blocks, LANES), jnp.float32),
        ),
        in_specs=[hbm] * 7 + [pl.BlockSpec(memory_space=pltpu.SMEM)],
        out_specs=(vmem,) * 5,
        scratch_shapes=[
            pltpu.VMEM((blocks, width), jnp.float32),
            pltpu.VMEM((MOMENTS, blocks, LANES), jnp.float32),
            pltpu.VMEM((1, blocks), jnp.int32),
            pltpu.VMEM((halos // LANES, LANES), jnp.int32),
            pltpu.VMEM((3, blocks), jnp.int32),
            pltpu.VMEM((1, blocks), jnp.int32),
            pltpu.SemaphoreType.DMA((3,)),
            pltpu.SemaphoreType.DMA((4,)),
        ],
        compiler_params=pltpu.CompilerParams(vmem_limit_bytes=16 * 1024 * 1024),
        name="moments",
    )(
        *map(
            held,
            (
                positions, velocities, masses, block_halo.reshape(1, blocks),
                home_slot.reshape(halos // LANES, LANES), block_shift, block_live.reshape(1, blocks),
            ),
        ),
        block_count,
    )
    recv = lax.all_to_all(send, AXES[::-1], 0, 0)
    table, kinetic, radial = pl.pallas_call(
        functools.partial(outputs_kernel, groups, domains, halos),
        out_shape=(
            jax.ShapeDtypeStruct((MOMENTS, halos // devices), jnp.float32),
            jax.ShapeDtypeStruct((blocks, width), jnp.float32),
            jax.ShapeDtypeStruct((blocks, width), jnp.float32),
        ),
        in_specs=[vmem] * 5,
        out_specs=(anywhere,) * 3,
        scratch_shapes=[
            pltpu.VMEM((MOMENTS, halos // devices), jnp.float32),
            pltpu.VMEM((blocks, width), jnp.float32),
            pltpu.VMEM((blocks, width), jnp.float32),
            pltpu.VMEM((blocks, 8), jnp.float32),
            pltpu.SemaphoreType.DMA((2, OUT_CHUNKS)),
            pltpu.SemaphoreType.DMA,
        ],
        compiler_params=pltpu.CompilerParams(vmem_limit_bytes=16 * 1024 * 1024),
        name="outputs",
    )(recv, pos, vel, side, cols)
    return table, kinetic, radial


def solution(mesh):
    return jax.shard_map(
        local,
        mesh=mesh,
        in_specs=(
            P(None, AXES, None), P(None, AXES, None), P(AXES, None), P(AXES),
            P(None, AXES), P(AXES), P(AXES), P(),
        ),
        out_specs=(P(None, AXES), P(AXES, None), P(AXES, None)),
        check_vma=False,
    )
```
